32 devices in a mesh: gz: 4 (over y, x), gy: 8 (over z, core).
Axes of the slice: x: 2, y: 2, z: 4, core: 2. Of those that a mesh axis runs over, the one named last changes fastest.
Arguments:
- grid_grad: float32 [64, 128, 512], P('gz', 'gy'), may hold values from -6 to 6
- cells: int32 [3, 65536], P(None, ('gz', 'gy')), may hold values from 0 to 511, as said below
- offsets: int32 [3, 65536], P(None, ('gz', 'gy')), may hold values from 0 to 1023
- owners: int32 [65536, 1], P(('gz', 'gy')), may hold values from 0 to 31; in each aligned block of 2048 rows (0 to 2047, 2048 to 4095, ...) at most 128 rows name the same one
- slots: int32 [65536], P(('gz', 'gy')), may hold values from 0 to 2047
Outputs:
- pos_grad: float32 [3, 65536], P(None, ('gz', 'gy'))
The draws below stay inside these ranges and needn't reach their ends.
Inputs may be any that keep to these rules, and one draw needn't show every extreme that they name: `cells`: the row's cell lies in the mesh block of the device that holds the row: along z in [gz * 16, gz * 16 + 16), along y in [gy * 16, gy * 16 + 16), where gz, gy are that device's indices. `owners`: owners are linear device indices gz * 8 + gy. Among the rows of one device, no owner is named by more than 128 rows; some owner is named by exactly 128.
All inputs are finite; a program needn't handle non-finite values.
Results may differ from the reference program's by a relative error of at most 0.0003.
Values sent between devices are 32-bit elements; how exact they have to be, the bound alone decides.
A program may use at most 64 MiB of HBM per device.

```python
import math
import jax
import jax.numpy as jnp
import numpy as np

CZ = 16
CY = 16
LX = 512
P_DEV = 2048
NZ = 64
NY = 128
PROWS = 65536
CAP = 128
N_GZ = 4
N_GY = 8
DEVICES = 32


def draw_cells(key, part):
    total_rows = P_DEV * N_GZ * N_GY
    device = jnp.arange(total_rows, dtype=jnp.int32) // P_DEV
    index_z = device // N_GY
    index_y = device % N_GY
    key_z = jax.random.fold_in(key, 11)
    key_y = jax.random.fold_in(key, 12)
    key_x = jax.random.fold_in(key, 13)
    cell_z = index_z * CZ + jax.random.randint(key_z, (total_rows,), 0, CZ, dtype=jnp.int32)
    cell_y = index_y * CY + jax.random.randint(key_y, (total_rows,), 0, CY, dtype=jnp.int32)
    cell_x = jax.random.randint(key_x, (total_rows,), 0, LX, dtype=jnp.int32)
    return jnp.stack([cell_z, cell_y, cell_x]).astype(jnp.int32)


def set_ends(result, rng, low, largest):
    extent = result.shape
    place = [jax.random.randint(jax.random.fold_in(rng, axis), (), 0, extent[axis]) for axis in range(len(extent))]
    result = result.at[tuple(place)].set(low)
    longest = extent.index(max(extent))
    place[longest] = (place[longest] + 1) % extent[longest]
    return result.at[tuple(place)].set(largest)


def levels(stream_key, shape, pieces, smallest, largest):
    def one(dim, shards_of):
        heights = jax.random.uniform(jax.random.fold_in(jax.random.fold_in(stream_key, 6), dim), (shards_of,), jnp.float32, smallest / len(pieces), largest / len(pieces))
        return jnp.repeat(jnp.exp(heights), shape[dim] // shards_of).reshape((-1,) + (1,) * (len(shape) - dim - 1))

    gain = one(*pieces[0])
    for cut in pieces[1:]:
        gain = gain * one(*cut)
    return gain


def shared_out(rng, own, number, rows, count, top, bound, lean):
    ranking = jax.random.permutation(rng, count)
    heavy_load, ordinary = load_shares(count, rows * top, bound, lean, True), load_shares(count, rows * top, bound, lean, False)
    places = jnp.arange(count)

    def named(sizes, rotation):
        used = int((sizes > 0).sum())
        fixed = max(1, used // 4)
        passed = fixed + (places - fixed + rotation * (used - fixed)) % max(1, count - fixed)
        return jnp.zeros((count,), jnp.int32).at[ranking[jnp.where(places < fixed, places, passed)]].set(jnp.asarray(sizes, jnp.int32))

    sizes = jnp.where(number % 4 == 0, named(heavy_load, number // 4), named(ordinary, number - number // 4 - 1))
    mixed = jax.random.permutation(jax.random.fold_in(own, 3), count)
    source_of, sink = mixed[0:count // 2 * 2:2], mixed[1:count // 2 * 2:2]
    room = jnp.minimum(sizes[source_of] - 1, bound - sizes[sink]) // 2
    room = jnp.where((source_of == ranking[0]) | (sink == ranking[0]) | (sizes[sink] == 0), 0, jnp.maximum(room, 0))
    passed = jax.random.randint(jax.random.fold_in(own, 4), (count // 2,), 0, 1 << 20) % (room + 1)
    sizes = sizes.at[source_of].add(-passed).at[sink].add(passed)
    members = jnp.searchsorted(jnp.cumsum(sizes), jnp.arange(rows * top), side="right").astype(jnp.int32)
    table = members.reshape(top, rows).T
    table = table[jax.random.permutation(jax.random.fold_in(own, 1), rows)]
    rotation = jax.random.randint(jax.random.fold_in(own, 2), (rows, 1), 0, top)
    return jnp.take_along_axis(table, (jnp.arange(top)[None, :] + rotation) % top, axis=1)


def load_shares(number_of, total, most, skew, full):
    loads = [(1 << 20) // math.isqrt(standing ** skew) + 1 for standing in range(1, number_of + 1)]
    largest = most if full else min(most, max(-(-total // number_of), total * loads[0] // sum(loads)))
    least = 1 if total - largest >= number_of - 1 else 0
    holding, surplus = [largest] + [least] * (number_of - 1), total - largest - least * (number_of - 1)
    while surplus > 0:
        free = [i for i in range(1, number_of) if holding[i] < largest] or [i for i in range(1, number_of) if holding[i] < most]
        pool, remaining = sum([loads[i] for i in free]), surplus
        for i in free:
            extra = min(most - holding[i], max(1, remaining * loads[i] // pool), surplus)
            holding[i] = holding[i] + extra
            surplus = surplus - extra
    return np.array(holding)


def scatter_about(stream_key, extent, spread, limit, pieces=(), kind=jnp.bfloat16):
    loudness = levels(stream_key, extent, pieces, -0.22, 0.18) if pieces else 1.0
    array = jax.random.normal(stream_key, extent, jnp.float32) * spread * loudness
    return jnp.minimum(jnp.maximum(array, -limit), limit).astype(kind)


def setup_inputs(seed: int = 0) -> dict:
    streams_of = jax.random.split(jax.random.key(seed), 6)
    grid_grad = scatter_about(streams_of[0], (NZ, NY, LX), 1.0, 6.0, ((0, 4), (1, 8)), jnp.float32)
    cells = draw_cells(jax.random.fold_in(streams_of[5], 71), 0)
    offsets = set_ends(jax.random.randint(streams_of[2], (3, PROWS), 0, 1024), jax.random.fold_in(streams_of[2], 1), 0, 1023).astype(jnp.int32)
    owners_keys = jax.random.split(jax.random.fold_in(streams_of[3], 1), PROWS // P_DEV)
    owners_turns = jax.random.permutation(jax.random.fold_in(streams_of[3], 3), PROWS // P_DEV)
    owners = jax.vmap(lambda own, number: shared_out(jax.random.fold_in(streams_of[3], 2), own, number, P_DEV, DEVICES, 1, CAP, 2))(owners_keys, owners_turns).reshape((PROWS, 1))
    slots = set_ends(jax.random.randint(streams_of[4], (PROWS,), 0, P_DEV), jax.random.fold_in(streams_of[4], 1), 0, P_DEV - 1).astype(jnp.int32)
    return {"grid_grad": grid_grad, "cells": cells, "offsets": offsets, "owners": owners, "slots": slots}


def cic_gradient(corner, fraction):
    weight_z = (1.0 - fraction[0], fraction[0])
    weight_y = (1.0 - fraction[1], fraction[1])
    weight_x = (1.0 - fraction[2], fraction[2])
    grad_z = jnp.zeros_like(fraction[0])
    grad_y = jnp.zeros_like(fraction[0])
    grad_x = jnp.zeros_like(fraction[0])
    for first in range(2):
        for second in range(2):
            grad_z = grad_z + (corner[1][first][second] - corner[0][first][second]) * weight_y[first] * weight_x[second]
            grad_y = grad_y + (corner[first][1][second] - corner[first][0][second]) * weight_z[first] * weight_x[second]
            grad_x = grad_x + (corner[first][second][1] - corner[first][second][0]) * weight_z[first] * weight_y[second]
    return jnp.stack([grad_z, grad_y, grad_x])


def reference(grid_grad, cells, offsets, owners, slots):
    size_z, size_y, size_x = grid_grad.shape
    fraction = (offsets.astype(jnp.float32) + 0.5) / 1024.0
    flat = grid_grad.reshape(-1)
    corner = []
    for step_z in range(2):
        plane = []
        for step_y in range(2):
            line = []
            for step_x in range(2):
                pos_z = (cells[0] + step_z) % size_z
                pos_y = (cells[1] + step_y) % size_y
                pos_x = (cells[2] + step_x) % size_x
                line.append(flat[(pos_z * size_y + pos_y) * size_x + pos_x])
            plane.append(line)
        corner.append(plane)
    gradient = cic_gradient(corner, fraction)
    target = (owners[:, 0] * P_DEV + slots).astype(jnp.int32)
    total = jnp.zeros((3, cells.shape[1]), jnp.float32)
    return total.at[:, target].add(gradient)
```

```python
import jax
import jax.numpy as jnp
from jax import lax
from jax.experimental import pallas as pl
from jax.experimental.pallas import tpu as pltpu
from jax.sharding import PartitionSpec as P

MESH = pl.DeviceIdType.MESH
BF = jnp.bfloat16
F32 = jnp.float32
LANES = 128


def iota(shape, axis):
    return lax.broadcasted_iota(jnp.int32, shape, axis)


def hot(mask):
    return jnp.where(mask, 1.0, 0.0).astype(BF)


def split(value):
    high = value.astype(BF)
    low = (value - high.astype(F32)).astype(BF)
    return high, low


def dot_nn(a, b):
    return lax.dot_general(a, b, (((1,), (0,)), ((), ())), preferred_element_type=F32)


def dot_nt(a, b):
    return lax.dot_general(a, b, (((1,), (1,)), ((), ())), preferred_element_type=F32)


def with_diff(rows):
    size_x = rows.shape[1]
    diff = pltpu.roll(rows, size_x - 1, 1) - rows
    return jnp.concatenate([*split(rows), *split(diff)], axis=0)


def thirds(value):
    high, rest = split(value)
    return high, rest, (value - high.astype(F32) - rest.astype(F32)).astype(BF)


def over(count, step, carry):
    if count == 1:
        return step(0, carry)
    return lax.fori_loop(0, count, step, carry)


def kernel(
    grid_ref, cells_ref, offsets_ref, owners_ref, slots_ref, out,
    cells, offsets, owners, slots, grid_v, row_s, halo_z, halo_y, mesh_s, low_x, base_s, rank_s, mine_s, early_s, later_s,
    early_r, later_r, place_s, high_s, load_sem, halo_send, halo_recv, early_send, early_recv, later_send, later_recv,
):
    count_z, count_y = lax.axis_size("gz"), lax.axis_size("gy")
    devices = count_z * count_y
    gz, gy = lax.axis_index("gz"), lax.axis_index("gy")
    me = gz * count_y + gy
    size_z, size_y, size_x = grid_ref.shape
    rows = cells.shape[1]
    chunk = min(256, rows)
    chunks = rows // chunk
    spans = [pl.ds(j * chunk, chunk) for j in range(chunks)]
    group = min(32, devices)
    groups = devices // group
    slab = size_z * size_y
    pieces_x = size_x // LANES
    fold = low_x.shape[0]
    folds = size_x // fold
    highs = rows // LANES

    loads = []
    for i, (source, target) in enumerate((
        (owners_ref, owners), (grid_ref, grid_v), (cells_ref, cells),
        (offsets_ref, offsets), (slots_ref, slots),
    )):
        loads.append(pltpu.make_async_copy(source, target, load_sem.at[i]))
        loads[-1].start()
    barrier = pltpu.get_barrier_semaphore()

    def each_other(act):
        few = devices <= 64

        def along_y(to_z, first):
            def step(shift, carry):
                act(to_z, lax.rem(gy + shift, count_y))
                return carry
            lax.fori_loop(first, count_y, step, 0, unroll=few)

        def step_z(shift, carry):
            along_y(lax.rem(gz + shift, count_z), 0)
            return carry
        along_y(gz, 1)
        lax.fori_loop(1, count_z, step_z, 0, unroll=few)

    def greet(to_z, to_y):
        pl.semaphore_signal(barrier, inc=1, device_id=(to_z, to_y), device_id_type=MESH)

    each_other(greet)

    for copy in loads:
        copy.wait()
    row_s[...] = grid_v[:, 0, :]
    mesh_s[...] = with_diff(grid_v[...].reshape(slab, size_x))
    corner = grid_v[0, 0:1, :]

    def place(span):
        cell = cells[:, span]
        frac = (offsets[:, span].astype(F32) + 0.5) / 1024.0
        return (cell[0:1] - gz * size_z, cell[1:2] - gy * size_y, cell[2:3],
                frac[0:1], frac[1:2], frac[2:3])

    def weights(size, cell, frac):
        at = iota((size, cell.shape[1]), 0)
        lower, upper = at == cell, at == cell + 1
        return (jnp.where(lower, 1.0 - frac, jnp.where(upper, frac, 0.0)),
                jnp.where(lower, -1.0, jnp.where(upper, 1.0, 0.0)))

    def by_four(first, second, third, fourth):
        part = lax.bitwise_and(iota((8, first.shape[1]), 0), 3)
        return jnp.where(part == 0, first, jnp.where(part == 1, second, jnp.where(part == 2, third, fourth)))

    def main_chunk(span):
        cz, cy, cx, fz, fy, fx = place(span)
        prod = dot_nn(mesh_s[...], hot(iota((size_x, chunk), 0) == cx))
        low_x[:, span] = hot(iota((fold, chunk), 0) == lax.bitwise_and(cx, fold - 1))
        z_at, z_frac = jnp.broadcast_to(cz, (8, chunk)), jnp.broadcast_to(fz, (8, chunk))
        gz0 = 1.0 - z_frac
        tiles = size_y // 8
        total = [[jnp.zeros((8, chunk), F32) for _ in range(tiles)] for _ in range(4)]
        for z in range(size_z):
            lower, upper = z_at == z, z_at == z - 1
            weight = jnp.where(lower, gz0, jnp.where(upper, z_frac, 0.0))
            diff = jnp.where(lower, -1.0, jnp.where(upper, 1.0, 0.0))
            for t in range(tiles):
                first = z * size_y + 8 * t
                at = [prod[q * slab + first:q * slab + first + 8] for q in range(4)]
                value, slope = at[0] + at[1], at[2] + at[3]
                total[0][t] += weight * value
                total[1][t] += diff * value
                total[2][t] += weight * slope
                total[3][t] += diff * slope
        a_w, a_d, b_w, b_d = (jnp.concatenate(t, axis=0) for t in total)
        w_y, d_y = weights(size_y, cy, fy)
        base_s[0:1, span] = jnp.sum((a_d + fx * b_d) * w_y, axis=0, keepdims=True)
        base_s[1:2, span] = jnp.sum((a_w + fx * b_w) * d_y, axis=0, keepdims=True)
        base_s[2:3, span] = jnp.sum(b_w * w_y, axis=0, keepdims=True)

    def top(cell, frac, size):
        at_top = cell == size - 1
        return jnp.where(at_top, frac, 0.0), jnp.where(at_top, 1.0, 0.0)

    def folded(planes):
        table = jnp.concatenate([with_diff(plane) for plane in planes], axis=0)
        return jnp.concatenate([table[:, f * fold:(f + 1) * fold] for f in range(folds)], axis=0)

    def summed(found, fx, w, d):
        size = found.shape[0] // 4
        value, slope = found[:size] + found[size:2 * size], found[2 * size:3 * size] + found[3 * size:]
        read = value + fx * slope
        return [jnp.sum(each, axis=0, keepdims=True) for each in (w * read, d * read, w * slope)]

    def with_halos(table, span):
        cz, cy, cx, fz, fy, fx = place(span)
        prod = dot_nn(table, low_x[:, span])
        count = table.shape[0] // folds
        which = lax.shift_right_logical(cx, fold.bit_length() - 1)
        found = prod[(folds - 1) * count:]
        for f in range(folds - 1):
            found = jnp.where(which == f, prod[f * count:(f + 1) * count], found)
        z_w, z_d, z_x = summed(found[:4 * size_y], fx, *weights(size_y, cy, fy))
        y_w, y_d, y_x = summed(found[4 * size_y:], fx, *weights(size_z, cz, fz))
        (wz, dz), (wy, dy) = top(cz, fz, size_z), top(cy, fy, size_y)
        return by_four(
            base_s[0:1, span] + (dz * z_w + wy * y_d), base_s[1:2, span] + (wz * z_d + dy * y_w),
            base_s[2:3, span] + (wz * z_x + wy * y_x), 0.0)

    def about(span):
        cz, cy, cx, fz, fy, fx = place(span)
        (wz, dz), (wy, dy) = top(cz, fz, size_z), top(cy, fy, size_y)
        return by_four((slots[:, span] + 1).astype(F32), cx.astype(F32) + fx, wz * dy, wy * dz)

    def pack(values, into, terms):
        wide = 2 * group
        parts = [terms(jnp.concatenate([value] * 2, axis=0)) for value in values]

        def pack_group(g, carry):
            total = jnp.zeros((len(parts[0]) * wide, 2 * LANES), F32)
            for part, span in zip(parts, spans):
                mask = mine_s[:, span] if groups == 1 else own_rows(g, span, chunk)
                left = jnp.concatenate([each * mask[r:r + 16] for each in part for r in range(0, wide, 16)], axis=0)
                total = total + dot_nt(left, rank_s[:, span])
            packed = total[:wide]
            for k in range(1, len(parts[0])):
                packed = packed + total[k * wide:(k + 1) * wide]
            for d in range(group):
                half, side = d // 2, d % 2 * LANES
                into[g * group + d, 0:4] = packed[4 * half:4 * half + 4, side:side + LANES]
            return carry

        over(groups, pack_group, 0)

    pl.semaphore_wait(barrier, devices - 1)
    below_z = lax.rem(gz + count_z - 1, count_z)
    below_y = lax.rem(gy + count_y - 1, count_y)
    halos = []
    for i, (source, target, device) in enumerate((
        (row_s, halo_y, (gz, below_y)),
        (grid_v.at[0], halo_z, (below_z, gy)),
    )):
        halos.append(pltpu.make_async_remote_copy(
            src_ref=source, dst_ref=target, send_sem=halo_send.at[i], recv_sem=halo_recv.at[i],
            device_id=device, device_id_type=MESH,
        ))
        halos[-1].start()

    def send_all(source, target, send_sem, recv_sem):
        def post(to_z, to_y):
            pltpu.make_async_remote_copy(
                src_ref=source.at[to_z * count_y + to_y], dst_ref=target.at[me], send_sem=send_sem, recv_sem=recv_sem,
                device_id=(to_z, to_y), device_id_type=MESH,
            ).start()

        first = min(2, count_y)
        for to_y in range(first):
            pl.when(me != to_y)(lambda to_y=to_y: post(0, to_y))

        def post_later(to_z, to_y):
            pl.when(to_z * count_y + to_y >= first)(lambda: post(to_z, to_y))

        each_other(post_later)

    def sent(source, target, send_sem, recv_sem, count):
        at = pl.ds(0, count)
        return pltpu.make_async_remote_copy(
            src_ref=source.at[at], dst_ref=target.at[at], send_sem=send_sem, recv_sem=recv_sem,
            device_id=(below_z, below_y), device_id_type=MESH,
        )

    owner = owners[...]
    before = hot(iota((chunk, chunk), 0) < iota((chunk, chunk), 1))

    def rank_group(g, ranks):
        mine = jnp.where(iota((group, rows), 0) + g * group == owner, 1.0, 0.0)
        pieces = [mine[:, c * chunk:(c + 1) * chunk] for c in range(chunks)]
        inside = dot_nn(jnp.concatenate(pieces, axis=0).astype(BF), before)
        start = jnp.zeros((group, 1), F32)
        found = []
        for c in range(chunks):
            where = inside[c * group:(c + 1) * group] + start
            found.append(jnp.sum(pieces[c] * where, axis=0, keepdims=True))
            start = start + jnp.sum(pieces[c], axis=1, keepdims=True)
        return ranks + jnp.concatenate(found, axis=1)

    ranks = over(groups, rank_group, jnp.zeros((1, rows), F32))
    odd = lax.bitwise_and(owner, 1)
    rank_s[...] = hot(iota((2 * LANES, rows), 0) == ranks.astype(jnp.int32) + odd * LANES)

    def own_rows(g, span, count):
        whose = lax.shift_right_logical(iota((2 * group, count), 0), 2) + g * (group // 2)
        return hot(whose == lax.shift_right_logical(owners[:, span], 1))

    if groups == 1:
        mine_s[...] = own_rows(0, pl.ds(0, rows), rows)

    early = chunks // 2
    for span in spans[:early]:
        main_chunk(span)
    pack([about(span) for span in spans], early_s, thirds)
    shared = [corner[:, k * LANES:(k + 1) * LANES] for k in range(pieces_x)]

    def share(d, carry):
        for k in range(pieces_x):
            early_s[d, 4 + k:5 + k] = shared[k]
        return carry

    lax.fori_loop(0, devices, share, 0, unroll=devices <= 64)

    send_all(early_s, early_r, early_send, early_recv)
    early_r[me] = early_s[me]

    for span in spans[early:]:
        main_chunk(span)

    for copy in halos:
        copy.wait()
    table = folded([halo_z[...], halo_y[...]])
    pack([with_halos(table, span) for span in spans], later_s, split)
    send_all(later_s, later_r, later_send, later_recv.at[gz])
    later_r[me] = later_s[me]

    sent(early_s, early_r, early_send, early_recv, devices - 1).wait()

    def from_corner(source):
        info = early_r[source]
        at_z, at_y = source // count_y, source % count_y
        if isinstance(source, int):
            other = (at_z + 1) % count_z * count_y + (at_y + 1) % count_y
        else:
            other = lax.rem(at_z + 1, count_z) * count_y + lax.rem(at_y + 1, count_y)
        row = early_r[other][4:]
        row = jnp.concatenate([row, row], axis=0) if pieces_x == 4 else row
        full = row.shape[0]
        where_x = jnp.broadcast_to(info[1:2], (full, LANES))
        cell = where_x.astype(jnp.int32)
        frac = where_x - cell.astype(F32)
        part = lax.bitwise_and(iota((full, LANES), 0), pieces_x - 1)

        def read(at):
            found = jnp.take_along_axis(row, lax.bitwise_and(at, LANES - 1), axis=1, mode="promise_in_bounds")
            found = jnp.where(part == lax.shift_right_logical(at, 7), found, 0.0)
            return jnp.sum(found[:pieces_x], axis=0, keepdims=True)

        low, high = read(cell), read(lax.bitwise_and(cell + 1, size_x - 1))
        slope = high - low
        value = low + frac[0:1] * slope
        wz, wy = info[2:3], info[3:4]
        return by_four(wy * value, wz * value, wz * wy * slope, 0.0)[:4]

    def where_to(blocks):
        record = jnp.concatenate([block[0:1] for block in blocks], axis=1).astype(jnp.int32) - 1
        width = record.shape[1]
        which = lax.shift_right_logical(iota((4 * highs, width), 0), 2)
        return (hot(iota((LANES, width), 0) == lax.bitwise_and(record, LANES - 1)),
                hot(which == lax.shift_right_arithmetic(record, 7)))

    def added(blocks, low_hot, high_hot):
        values = jnp.concatenate(blocks, axis=1)
        halves = split(jnp.concatenate([values] * 4, axis=0))
        left = jnp.concatenate([half * high_hot[r:r + 16] for half in halves for r in range(0, 4 * highs, 16)], axis=0)
        total = dot_nt(left, low_hot)
        return total[:4 * highs] + total[4 * highs:]

    if groups == 1:
        low_hot, high_hot = where_to([early_r[d] for d in range(devices)])
        place_s[...] = low_hot
        high_s[...] = high_hot
        total = added([from_corner(d) for d in range(devices)], low_hot, high_hot)
    else:
        def corner_group(g, total):
            low_hot, high_hot = where_to([early_r[g * group + d] for d in range(group)])
            return total + added([from_corner(g * group + d) for d in range(group)], low_hot, high_hot)

        total = over(groups, corner_group, jnp.zeros((4 * highs, LANES), F32))

    for shift in [*range(1, count_z - 1), 0, *range(max(1, count_z - 1), count_z)]:
        from_z = lax.rem(gz + shift, count_z)
        sent(later_s, later_r, later_send, later_recv.at[from_z], count_y if shift else count_y - 1).wait_recv()
        if groups == 1:
            first = from_z * count_y
            width = count_y * LANES
            at = pl.ds(pl.multiple_of(first * LANES, width), width)
            total = total + added([later_r[first + d] for d in range(count_y)], place_s[:, at], high_s[:, at])
    sent(later_s, later_r, later_send, later_recv.at[gz], devices - 1).wait_send()
    if groups > 1:
        def add_group(g, total):
            low_hot, high_hot = where_to([early_r[g * group + d] for d in range(group)])
            return total + added([later_r[g * group + d] for d in range(group)], low_hot, high_hot)

        total = over(groups, add_group, total)
    for h in range(highs):
        out[:, h * LANES:(h + 1) * LANES] = total[4 * h:4 * h + 3]


def body(grid_grad, cells, offsets, owners, slots):
    size_z, size_y, size_x = grid_grad.shape
    rows = cells.shape[1]
    count_z = lax.axis_size("gz")
    devices = count_z * lax.axis_size("gy")
    group = min(32, devices)
    width = devices * LANES if devices == group else LANES
    vmem = pl.BlockSpec(memory_space=pltpu.VMEM)
    hbm = pl.BlockSpec(memory_space=pltpu.HBM)
    return pl.pallas_call(
        kernel,
        out_shape=pltpu.VMEM((3, rows), F32),
        in_specs=[hbm] * 5,
        out_specs=vmem,
        scratch_shapes=[
            pltpu.VMEM((3, rows), jnp.int32),
            pltpu.VMEM((3, rows), jnp.int32),
            pltpu.VMEM((1, rows), jnp.int32),
            pltpu.VMEM((1, rows), jnp.int32),
            pltpu.VMEM((size_z, size_y, size_x), F32),
            pltpu.VMEM((size_z, size_x), F32),
            pltpu.VMEM((size_y, size_x), F32),
            pltpu.VMEM((size_z, size_x), F32),
            pltpu.VMEM((4 * size_z * size_y, size_x), BF),
            pltpu.VMEM((min(256, size_x), rows), BF),
            pltpu.VMEM((8, rows), F32),
            pltpu.VMEM((2 * LANES, rows), BF),
            pltpu.VMEM((2 * group, rows), BF),
            pltpu.VMEM((devices, 4 + size_x // LANES, LANES), F32),
            pltpu.VMEM((devices, 4, LANES), F32),
            pltpu.VMEM((devices, 4 + size_x // LANES, LANES), F32),
            pltpu.VMEM((devices, 4, LANES), F32),
            pltpu.VMEM((LANES, width), BF),
            pltpu.VMEM((4 * rows // LANES, width), BF),
            pltpu.SemaphoreType.DMA((5,)),
            pltpu.SemaphoreType.DMA((2,)),
            pltpu.SemaphoreType.DMA((2,)),
            pltpu.SemaphoreType.DMA,
            pltpu.SemaphoreType.DMA,
            pltpu.SemaphoreType.DMA,
            pltpu.SemaphoreType.DMA((count_z,)),
        ],
        compiler_params=pltpu.CompilerParams(collective_id=0, has_side_effects=True, vmem_limit_bytes=56 * 1024 * 1024),
        name="cic",
    )(grid_grad, cells, offsets, owners.reshape(1, rows), slots.reshape(1, rows))


def solution(mesh):
    placed = (
        P("gz", "gy", None),
        P(None, ("gz", "gy")),
        P(None, ("gz", "gy")),
        P(("gz", "gy"), None),
        P(("gz", "gy")),
    )
    return jax.shard_map(
        body, mesh=mesh, in_specs=placed, out_specs=P(None, ("gz", "gy")), check_vma=False
    )
```

```python
import jax
import jax.numpy as jnp
from jax import lax
from jax.experimental import pallas as pl
from jax.experimental.pallas import tpu as pltpu
from jax.sharding import PartitionSpec as P

MESH = pl.DeviceIdType.MESH
BF = jnp.bfloat16
F32 = jnp.float32
LANES = 128


def iota(shape, axis):
    return lax.broadcasted_iota(jnp.int32, shape, axis)


def hot(mask):
    return jnp.where(mask, 1.0, 0.0).astype(BF)


def split(value):
    high = value.astype(BF)
    low = (value - high.astype(F32)).astype(BF)
    return high, low


def dot_nn(a, b):
    return lax.dot_general(a, b, (((1,), (0,)), ((), ())), preferred_element_type=F32)


def dot_nt(a, b):
    return lax.dot_general(a, b, (((1,), (1,)), ((), ())), preferred_element_type=F32)


def with_diff(rows):
    size_x = rows.shape[1]
    diff = pltpu.roll(rows, size_x - 1, 1) - rows
    return jnp.concatenate([*split(rows), *split(diff)], axis=0)


def hot_at(size, value, shift=0):
    value = jnp.broadcast_to(value.astype(F32), (16, value.shape[1])).astype(BF)
    at = lax.shift_right_logical(iota(value.shape, 0), shift).astype(F32)
    one, none = jnp.ones(value.shape, BF), jnp.zeros(value.shape, BF)
    return jnp.concatenate(
        [jnp.where((at + float(k >> shift)).astype(BF) == value, one, none) for k in range(0, size, 16)], axis=0)


def thirds(value):
    high, rest = split(value)
    return high, rest, (value - high.astype(F32) - rest.astype(F32)).astype(BF)


def over(count, step, carry):
    if count == 1:
        return step(0, carry)
    return lax.fori_loop(0, count, step, carry)


def kernel(
    grid_ref, cells_ref, offsets_ref, owners_ref, slots_ref, out,
    cells, offsets, owners, slots, grid_v, row_s, halo_s, mesh_s, low_x, base_s, last_s, rank_s, rank_t, mine_s, early_s, later_s,
    first_s,
    early_r, later_r, place_s, high_s, load_sem, halo_send, halo_recv, early_send, early_recv, later_send, later_recv,
):
    count_z, count_y = lax.axis_size("gz"), lax.axis_size("gy")
    devices = count_z * count_y
    gz, gy = lax.axis_index("gz"), lax.axis_index("gy")
    me = gz * count_y + gy
    size_z, size_y, size_x = grid_ref.shape
    rows = cells.shape[1]
    chunk = min(256, rows)
    chunks = rows // chunk
    spans = [pl.ds(j * chunk, chunk) for j in range(chunks)]
    group = min(32, devices)
    groups = devices // group
    slab = size_z * size_y
    pieces_x = size_x // LANES
    fold = low_x.shape[0]
    folds = size_x // fold
    highs = rows // LANES

    loads = []
    for i, (source, target) in enumerate((
        (owners_ref, owners), (grid_ref, grid_v), (cells_ref, cells), (offsets_ref, offsets), (slots_ref, slots),
    )):
        loads.append(pltpu.make_async_copy(source, target, load_sem.at[i]))
        loads[-1].start()
    barrier = pltpu.get_barrier_semaphore()

    def each_other(act):
        few = devices <= 64

        def along_y(to_z, first):
            def step(shift, carry):
                act(to_z, lax.rem(gy + shift, count_y))
                return carry
            lax.fori_loop(first, count_y, step, 0, unroll=few)

        def step_z(shift, carry):
            along_y(lax.rem(gz + shift, count_z), 0)
            return carry
        along_y(gz, 1)
        lax.fori_loop(1, count_z, step_z, 0, unroll=few)

    def greet(to_z, to_y):
        pl.semaphore_signal(barrier, inc=1, device_id=(to_z, to_y), device_id_type=MESH)

    each_other(greet)

    loads[0].wait()
    owner = owners[...]
    before = hot(iota((chunk, chunk), 0) < iota((chunk, chunk), 1))

    def rank_group(g, ranks):
        mine = jnp.where(iota((group, rows), 0) + g * group == owner, 1.0, 0.0)
        pieces = [mine[:, c * chunk:(c + 1) * chunk] for c in range(chunks)]
        inside = dot_nn(jnp.concatenate(pieces, axis=0).astype(BF), before)
        start = jnp.zeros((group, 1), F32)
        found = []
        for c in range(chunks):
            where = inside[c * group:(c + 1) * group] + start
            found.append(jnp.sum(pieces[c] * where, axis=0, keepdims=True))
            start = start + jnp.sum(pieces[c], axis=1, keepdims=True)
        return ranks + jnp.concatenate(found, axis=1)

    ranks = over(groups, rank_group, jnp.zeros((1, rows), F32))
    odd = lax.bitwise_and(owner, 1)
    rank_s[...] = hot_at(2 * LANES, ranks + (odd * LANES).astype(F32))

    def own_rows(g, span):
        return hot_at(2 * group, lax.shift_right_logical(owners[:, span], 1) - g * (group // 2), 2)

    if groups == 1:
        mine_s[...] = own_rows(0, pl.ds(0, rows))

    for copy in loads[1:]:
        copy.wait()
    row_s[...] = grid_v[:, 0, :]
    mesh_s[...] = with_diff(grid_v[...].reshape(slab, size_x))
    corner = grid_v[0, 0:1, :]

    def place(span):
        cell = cells[:, span]
        frac = (offsets[:, span].astype(F32) + 0.5) / 1024.0
        return (cell[0:1] - gz * size_z, cell[1:2] - gy * size_y, cell[2:3],
                frac[0:1], frac[1:2], frac[2:3])

    def weights(size, cell, frac):
        at = iota((size, cell.shape[1]), 0)
        lower, upper = at == cell, at == cell + 1
        return (jnp.where(lower, 1.0 - frac, jnp.where(upper, frac, 0.0)),
                jnp.where(lower, -1.0, jnp.where(upper, 1.0, 0.0)))

    def by_four(first, second, third, fourth):
        part = lax.bitwise_and(iota((8, first.shape[1]), 0), 3)
        return jnp.where(part == 0, first, jnp.where(part == 1, second, jnp.where(part == 2, third, fourth)))

    def main_chunk(span):
        cz, cy, cx, fz, fy, fx = place(span)
        which, low = lax.shift_right_logical(cx, fold.bit_length() - 1), lax.bitwise_and(cx, fold - 1)
        low_x[:, span] = hot_at(fold, low)
        prod = dot_nn(mesh_s[...], jnp.concatenate(
            [hot_at(fold, jnp.where(which == f, low, -1)) for f in range(folds)], axis=0))
        z_at, z_frac = jnp.broadcast_to(cz, (8, chunk)), jnp.broadcast_to(fz, (8, chunk))
        gz0 = 1.0 - z_frac
        tiles = size_y // 8
        total = [[jnp.zeros((8, chunk), F32) for _ in range(tiles)] for _ in range(4)]
        for z in range(size_z):
            lower, upper = z_at == z, z_at == z - 1
            weight = jnp.where(lower, gz0, jnp.where(upper, z_frac, 0.0))
            diff = jnp.where(lower, -1.0, jnp.where(upper, 1.0, 0.0))
            for t in range(tiles):
                first = z * size_y + 8 * t
                at = [prod[q * slab + first:q * slab + first + 8] for q in range(4)]
                value, slope = at[0] + at[1], at[2] + at[3]
                total[0][t] += weight * value
                total[1][t] += diff * value
                total[2][t] += weight * slope
                total[3][t] += diff * slope
        w_y, d_y = weights(size_y, cy, fy)
        sums = [0.0, 0.0, 0.0]
        for t in range(tiles):
            a_w, a_d, b_w, b_d = (total[q][t] for q in range(4))
            w, d = w_y[8 * t:8 * t + 8], d_y[8 * t:8 * t + 8]
            sums = [sums[0] + (a_d + fx * b_d) * w, sums[1] + (a_w + fx * b_w) * d, sums[2] + b_w * w]
        for q in range(3):
            base_s[q, :, span] = sums[q]

    def top(cell, frac, size):
        at_top = cell == size - 1
        return jnp.where(at_top, frac, 0.0), jnp.where(at_top, 1.0, 0.0)

    def folded(plane):
        table = with_diff(plane)
        return jnp.concatenate([table[:, f * fold:(f + 1) * fold] for f in range(folds)], axis=0)

    def by_rows(first, second, third):
        row = iota(first.shape, 0)
        even, lower = lax.bitwise_and(row, 1) == 0, lax.bitwise_and(row, 2) == 0
        pair = jnp.where(even, first, second) + pltpu.roll(jnp.where(even, second, first), 1, 0)
        third = third + pltpu.roll(third, 1, 0)
        third = jnp.where(even, third, 0.0)
        both = jnp.where(lower, pair, third) + pltpu.roll(jnp.where(lower, third, pair), 2, 0)
        return both + pltpu.roll(both, 4, 0)

    def either(first, one, other):
        if isinstance(first, bool):
            return one if first else other
        return jnp.where(first, one, other)

    def halo_weights(span, along_y):
        cz, cy, cx, fz, fy, fx = place(span)
        size = either(along_y, size_y, size_z) if isinstance(along_y, bool) else size_y
        w, d = weights(size, either(along_y, cy, cz), either(along_y, fy, fz))
        w_top, d_top = top(either(along_y, cz, cy), either(along_y, fz, fy), either(along_y, size_z, size_y))
        across, beside = d_top * w, w_top * d
        return either(along_y, across, beside), either(along_y, beside, across), w_top * w

    def halo_sums(table, span, factors):
        cx, fx = place(span)[2::3]
        prod = dot_nn(table, low_x[:, span])
        count = table.shape[0] // folds
        size = count // 4
        which = lax.shift_right_logical(cx, fold.bit_length() - 1)

        def found(first):
            pick = None
            for f in reversed(range(folds)):
                at = f * count + first
                part = prod[at:at + size] + prod[at + size:at + 2 * size]
                pick = part if pick is None else jnp.where(which == f, part, pick)
            return pick

        value, slope = found(0), found(2 * size)
        read = value + fx * slope
        parts = (factors[0] * read, factors[1] * read, factors[2] * slope)
        sums = []
        for q in range(3):
            total = base_s[q, :, span]
            for t in range(0, size, 8):
                total = total + parts[q][t:t + 8]
            sums.append(total)
        return sums

    def about(span):
        cz, cy, cx, fz, fy, fx = place(span)
        (wz, dz), (wy, dy) = top(cz, fz, size_z), top(cy, fy, size_y)
        return by_four((slots[:, span] + 1).astype(F32), cx.astype(F32) + fx, wz * dy, wy * dz)

    def pack_rows(g, parts, wide, ranked):
        total = jnp.zeros((len(parts[0]) * wide, 2 * LANES), F32)
        for part, span in zip(parts, spans):
            mask = mine_s[:, span] if groups == 1 else own_rows(g, span)
            left = jnp.concatenate([each * mask[r:r + 16] for each in part for r in range(0, wide, 16)], axis=0)
            total = total + ranked(left, span)
        packed = total[:wide]
        for k in range(1, len(parts[0])):
            packed = packed + total[k * wide:(k + 1) * wide]
        return packed

    def keep(packed, into, first):
        for d in range(packed.shape[0] // 2):
            half, side = d // 2, d % 2 * LANES
            into[first + d, 0:4] = packed[4 * half:4 * half + 4, side:side + LANES]

    def pack(parts, into, ranked):
        def pack_group(g, carry):
            keep(pack_rows(g, parts, 2 * group, ranked), into, g * group)
            return carry

        over(groups, pack_group, 0)

    def by_rank(left, span):
        return dot_nt(left, rank_s[:, span])

    def by_rank_t(left, span):
        return dot_nn(left, rank_t[span])

    def terms_of(value, terms):
        return terms(jnp.concatenate([value] * 2, axis=0))

    pl.semaphore_wait(barrier, devices - 1)
    below_z = lax.rem(gz + count_z - 1, count_z)
    below_y = lax.rem(gy + count_y - 1, count_y)
    halos = []
    for i, (source, target, device) in enumerate((
        (row_s, halo_s.at[0, 0:size_z], (gz, below_y)),
        (grid_v.at[0], halo_s.at[1, 0:size_y], (below_z, gy)),
    )):
        halos.append(pltpu.make_async_remote_copy(
            src_ref=source, dst_ref=target, send_sem=halo_send.at[i], recv_sem=halo_recv.at[i],
            device_id=device, device_id_type=MESH,
        ))
        halos[-1].start()

    def post(source, target, send_sem, recv_sem, device):
        pltpu.make_async_remote_copy(
            src_ref=source, dst_ref=target.at[me], send_sem=send_sem, recv_sem=recv_sem,
            device_id=device, device_id_type=MESH,
        ).start()

    first_few = min(2, count_y)

    def post_first(source, *where):
        for to_y in range(first_few):
            pl.when(me != to_y)(lambda to_y=to_y: post(source.at[to_y], *where, (0, to_y)))

    def post_rest(source, *where):
        def one(to_z, to_y):
            other = to_z * count_y + to_y
            pl.when(other >= first_few)(lambda: post(source.at[other], *where, (to_z, to_y)))

        each_other(one)

    def sent(source, target, send_sem, recv_sem, count):
        at = pl.ds(0, count)
        return pltpu.make_async_remote_copy(
            src_ref=source.at[at], dst_ref=target.at[at], send_sem=send_sem, recv_sem=recv_sem,
            device_id=(below_z, below_y), device_id_type=MESH,
        )

    early = chunks // 2
    for span in spans[:early]:
        main_chunk(span)
    pack([terms_of(about(span), thirds) for span in spans], early_s, by_rank)
    shared = [corner[:, k * LANES:(k + 1) * LANES] for k in range(pieces_x)]

    def share(d, carry):
        for k in range(pieces_x):
            early_s[d, 4 + k:5 + k] = shared[k]
        return carry

    lax.fori_loop(0, devices, share, 0, unroll=devices <= 64)

    post_first(early_s, early_r, early_send, early_recv)
    post_rest(early_s, early_r, early_send, early_recv)
    early_r[me] = early_s[me]

    for span in spans:
        rank_t[span] = rank_s[:, span].T
    for span in spans[early:]:
        main_chunk(span)

    at_end = lax.div(gy + 1, count_y)
    y_last = at_end == 1 if size_z == size_y else True
    y_copy, z_copy = halos

    def wait_for(first):
        if isinstance(first, bool):
            (z_copy if first else y_copy).wait()
        else:
            pl.when(first)(z_copy.wait)
            pl.when(jnp.logical_not(first))(y_copy.wait)

    def plane(along_y):
        if isinstance(along_y, bool):
            return folded(halo_s[1, 0:size_y] if along_y else halo_s[0, 0:size_z])
        return folded(halo_s[at_end if along_y is y_last else 1 - at_end])

    y_first = not y_last if isinstance(y_last, bool) else jnp.logical_not(y_last)
    wait_for(y_last)
    table = plane(y_last)
    for span in spans:
        sums = halo_sums(table, span, halo_weights(span, y_last))
        for q in range(3):
            base_s[q, :, span] = sums[q]
        for q, factor in enumerate(halo_weights(span, y_first)):
            last_s[q, :, span] = factor
    wait_for(y_first)
    table = plane(y_first)
    parts = [
        terms_of(by_rows(*halo_sums(table, span, [last_s[q, :, span] for q in range(3)])), split) for span in spans
    ]
    keep(pack_rows(0, parts, 16, by_rank_t), first_s, 0)
    post_first(first_s, later_r, later_send, later_recv.at[lax.div(gy, 2)])
    pack(parts, later_s, by_rank_t)
    post_rest(later_s, later_r, later_send, later_recv.at[lax.div(gy, 2)])
    later_r[me] = later_s[me]

    sent(early_s, early_r, early_send, early_recv, devices - 1).wait()

    def from_corner(source):
        info = early_r[source]
        at_z, at_y = source // count_y, source % count_y
        if isinstance(source, int):
            other = (at_z + 1) % count_z * count_y + (at_y + 1) % count_y
        else:
            other = lax.rem(at_z + 1, count_z) * count_y + lax.rem(at_y + 1, count_y)
        row = early_r[other][4:]
        row = jnp.concatenate([row, row], axis=0) if pieces_x == 4 else row
        full = row.shape[0]
        where_x = jnp.broadcast_to(info[1:2], (full, LANES))
        cell = where_x.astype(jnp.int32)
        frac = where_x - cell.astype(F32)
        part = lax.bitwise_and(iota((full, LANES), 0), pieces_x - 1)

        def read(at):
            found = jnp.take_along_axis(row, lax.bitwise_and(at, LANES - 1), axis=1, mode="promise_in_bounds")
            found = jnp.where(part == lax.shift_right_logical(at, 7), found, 0.0)
            return jnp.sum(found[:pieces_x], axis=0, keepdims=True)

        low, high = read(cell), read(lax.bitwise_and(cell + 1, size_x - 1))
        slope = high - low
        value = low + frac[0:1] * slope
        wz, wy = info[2:3], info[3:4]
        return by_four(wy * value, wz * value, wz * wy * slope, 0.0)[:4]

    def where_to(blocks):
        record = jnp.concatenate([block[0:1] for block in blocks], axis=1).astype(jnp.int32) - 1
        return (hot_at(LANES, lax.bitwise_and(record, LANES - 1)),
                hot_at(4 * highs, lax.shift_right_arithmetic(record, 7), 2))

    def added(blocks, low_hot, high_hot):
        values = jnp.concatenate(blocks, axis=1)
        halves = split(jnp.concatenate([values] * 4, axis=0))
        left = jnp.concatenate([half * high_hot[r:r + 16] for half in halves for r in range(0, 4 * highs, 16)], axis=0)
        total = dot_nt(left, low_hot)
        return total[:4 * highs] + total[4 * highs:]

    order = [z * count_y + y for first in range(0, count_y, 2) for z in range(count_z) for y in (first, first + 1)]
    if groups == 1:
        low_hot, high_hot = where_to([early_r[d] for d in order])
        place_s[...] = low_hot
        high_s[...] = high_hot
        total = added([from_corner(d) for d in order], low_hot, high_hot)
    else:
        def corner_group(g, total):
            low_hot, high_hot = where_to([early_r[g * group + d] for d in range(group)])
            return total + added([from_corner(g * group + d) for d in range(group)], low_hot, high_hot)

        total = over(groups, corner_group, jnp.zeros((4 * highs, LANES), F32))

    batch = 2 * count_z
    for part in range(count_y // 2):
        def wait_for_batch(count):
            sent(later_s, later_r, later_send, later_recv.at[part], count).wait_recv()

        pl.when(lax.div(gy, 2) == part)(lambda: wait_for_batch(batch - 1))
        pl.when(lax.div(gy, 2) != part)(lambda: wait_for_batch(batch))
        if groups == 1:
            at = slice(part * batch * LANES, (part + 1) * batch * LANES)
            sources = order[part * batch:(part + 1) * batch]
            total = total + added([later_r[d] for d in sources], place_s[:, at], high_s[:, at])
    sent(later_s, later_r, later_send, later_recv.at[0], devices - 1).wait_send()
    if groups > 1:
        def add_group(g, total):
            low_hot, high_hot = where_to([early_r[g * group + d] for d in range(group)])
            return total + added([later_r[g * group + d] for d in range(group)], low_hot, high_hot)

        total = over(groups, add_group, total)
    for h in range(highs):
        out[:, h * LANES:(h + 1) * LANES] = total[4 * h:4 * h + 3]


def body(grid_grad, cells, offsets, owners, slots):
    size_z, size_y, size_x = grid_grad.shape
    rows = cells.shape[1]
    count_y = lax.axis_size("gy")
    devices = lax.axis_size("gz") * count_y
    group = min(32, devices)
    width = devices * LANES if devices == group else LANES
    vmem = pl.BlockSpec(memory_space=pltpu.VMEM)
    hbm = pl.BlockSpec(memory_space=pltpu.HBM)
    return pl.pallas_call(
        kernel,
        out_shape=pltpu.VMEM((3, rows), F32),
        in_specs=[hbm] * 5,
        out_specs=vmem,
        scratch_shapes=[
            pltpu.VMEM((3, rows), jnp.int32),
            pltpu.VMEM((3, rows), jnp.int32),
            pltpu.VMEM((1, rows), jnp.int32),
            pltpu.VMEM((1, rows), jnp.int32),
            pltpu.VMEM((size_z, size_y, size_x), F32),
            pltpu.VMEM((size_z, size_x), F32),
            pltpu.VMEM((2, max(size_z, size_y), size_x), F32),
            pltpu.VMEM((4 * size_z * size_y, size_x), BF),
            pltpu.VMEM((min(256, size_x), rows), BF),
            pltpu.VMEM((3, 8, rows), F32),
            pltpu.VMEM((3, size_z, rows), F32),
            pltpu.VMEM((2 * LANES, rows), BF),
            pltpu.VMEM((rows, 2 * LANES), BF),
            pltpu.VMEM((2 * group, rows), BF),
            pltpu.VMEM((devices, 4 + size_x // LANES, LANES), F32),
            pltpu.VMEM((devices, 4, LANES), F32),
            pltpu.VMEM((8, 4, LANES), F32),
            pltpu.VMEM((devices, 4 + size_x // LANES, LANES), F32),
            pltpu.VMEM((devices, 4, LANES), F32),
            pltpu.VMEM((LANES, width), BF),
            pltpu.VMEM((4 * rows // LANES, width), BF),
            pltpu.SemaphoreType.DMA((5,)),
            pltpu.SemaphoreType.DMA((2,)),
            pltpu.SemaphoreType.DMA((2,)),
            pltpu.SemaphoreType.DMA,
            pltpu.SemaphoreType.DMA,
            pltpu.SemaphoreType.DMA,
            pltpu.SemaphoreType.DMA((count_y // 2,)),
        ],
        compiler_params=pltpu.CompilerParams(collective_id=0, has_side_effects=True, vmem_limit_bytes=56 * 1024 * 1024),
        name="cic",
    )(grid_grad, cells, offsets, owners.reshape(1, rows), slots.reshape(1, rows))


def solution(mesh):
    placed = (
        P("gz", "gy", None),
        P(None, ("gz", "gy")),
        P(None, ("gz", "gy")),
        P(("gz", "gy"), None),
        P(("gz", "gy")),
    )
    return jax.shard_map(
        body, mesh=mesh, in_specs=placed, out_specs=P(None, ("gz", "gy")), check_vma=False
    )
```

```python
import jax
import jax.numpy as jnp
from jax import lax
from jax.experimental import pallas as pl
from jax.experimental.pallas import tpu as pltpu
from jax.sharding import PartitionSpec as P

MESH = pl.DeviceIdType.MESH
BF = jnp.bfloat16
F32 = jnp.float32
LANES = 128


def iota(shape, axis):
    return lax.broadcasted_iota(jnp.int32, shape, axis)


def hot(mask):
    return jnp.where(mask, 1.0, 0.0).astype(BF)


def split(value):
    high = value.astype(BF)
    low = (value - high.astype(F32)).astype(BF)
    return high, low


def dot_nn(a, b):
    return lax.dot_general(a, b, (((1,), (0,)), ((), ())), preferred_element_type=F32)


def dot_nt(a, b):
    return lax.dot_general(a, b, (((1,), (1,)), ((), ())), preferred_element_type=F32)


def with_diff(rows):
    size_x = rows.shape[1]
    diff = pltpu.roll(rows, size_x - 1, 1) - rows
    return jnp.concatenate([*split(rows), *split(diff)], axis=0)


def hot_at(size, value, shift=0):
    value = jnp.broadcast_to(value.astype(F32), (16, value.shape[1])).astype(BF)
    at = lax.shift_right_logical(iota(value.shape, 0), shift).astype(F32)
    one, none = jnp.ones(value.shape, BF), jnp.zeros(value.shape, BF)
    return jnp.concatenate(
        [jnp.where((at + float(k >> shift)).astype(BF) == value, one, none) for k in range(0, size, 16)], axis=0)


def thirds(value):
    high, rest = split(value)
    return high, rest, (value - high.astype(F32) - rest.astype(F32)).astype(BF)


def over(count, step, carry):
    if count == 1:
        return step(0, carry)
    return lax.fori_loop(0, count, step, carry)


def kernel(
    grid_ref, cells_ref, offsets_ref, owners_ref, slots_ref, out,
    cells, offsets, owners, slots, grid_v, row_s, halo_s, mesh_s, low_x, base_s, last_s, rank_s, rank_t, mine_s, early_s, later_s,
    first_s,
    early_r, later_r, place_s, high_s, load_sem, halo_send, halo_recv, early_send, early_recv, later_send, later_recv,
):
    count_z, count_y = lax.axis_size("gz"), lax.axis_size("gy")
    devices = count_z * count_y
    gz, gy = lax.axis_index("gz"), lax.axis_index("gy")
    me = gz * count_y + gy
    size_z, size_y, size_x = grid_ref.shape
    rows = cells.shape[1]
    chunk = min(256, rows)
    chunks = rows // chunk
    spans = [pl.ds(j * chunk, chunk) for j in range(chunks)]
    group = min(32, devices)
    groups = devices // group
    slab = size_z * size_y
    pieces_x = size_x // LANES
    fold = low_x.shape[0]
    folds = size_x // fold
    highs = rows // LANES

    loads = []
    for i, (source, target) in enumerate((
        (owners_ref, owners), (grid_ref, grid_v), (cells_ref, cells), (offsets_ref, offsets), (slots_ref, slots),
    )):
        loads.append(pltpu.make_async_copy(source, target, load_sem.at[i]))
        loads[-1].start()
    barrier = pltpu.get_barrier_semaphore()

    def each_other(act):
        few = devices <= 64

        def along_y(to_z, first):
            def step(shift, carry):
                act(to_z, lax.rem(gy + shift, count_y))
                return carry
            lax.fori_loop(first, count_y, step, 0, unroll=few)

        def step_z(shift, carry):
            along_y(lax.rem(gz + shift, count_z), 0)
            return carry
        along_y(gz, 1)
        lax.fori_loop(1, count_z, step_z, 0, unroll=few)

    def greet(to_z, to_y):
        pl.semaphore_signal(barrier, inc=1, device_id=(to_z, to_y), device_id_type=MESH)

    each_other(greet)

    loads[0].wait()
    owner = owners[...]
    before = hot(iota((chunk, chunk), 0) < iota((chunk, chunk), 1))

    def rank_group(g, ranks):
        mine = jnp.where(iota((group, rows), 0) + g * group == owner, 1.0, 0.0)
        pieces = [mine[:, c * chunk:(c + 1) * chunk] for c in range(chunks)]
        inside = dot_nn(jnp.concatenate(pieces, axis=0).astype(BF), before)
        start = jnp.zeros((group, 1), F32)
        found = []
        for c in range(chunks):
            where = inside[c * group:(c + 1) * group] + start
            found.append(jnp.sum(pieces[c] * where, axis=0, keepdims=True))
            start = start + jnp.sum(pieces[c], axis=1, keepdims=True)
        return ranks + jnp.concatenate(found, axis=1)

    ranks = over(groups, rank_group, jnp.zeros((1, rows), F32))
    odd = lax.bitwise_and(owner, 1)
    rank_s[...] = hot_at(2 * LANES, ranks + (odd * LANES).astype(F32))

    def own_rows(g, span):
        return hot_at(2 * group, lax.shift_right_logical(owners[:, span], 1) - g * (group // 2), 2)

    if groups == 1:
        mine_s[...] = own_rows(0, pl.ds(0, rows))

    for copy in loads[1:]:
        copy.wait()
    row_s[...] = grid_v[:, 0, :]
    mesh_s[...] = with_diff(grid_v[...].reshape(slab, size_x))
    corner = grid_v[0, 0:1, :]

    def place(span):
        cell = cells[:, span]
        frac = (offsets[:, span].astype(F32) + 0.5) / 1024.0
        return (cell[0:1] - gz * size_z, cell[1:2] - gy * size_y, cell[2:3],
                frac[0:1], frac[1:2], frac[2:3])

    def weights(size, cell, frac):
        at = iota((size, cell.shape[1]), 0)
        lower, upper = at == cell, at == cell + 1
        return (jnp.where(lower, 1.0 - frac, jnp.where(upper, frac, 0.0)),
                jnp.where(lower, -1.0, jnp.where(upper, 1.0, 0.0)))

    def by_four(first, second, third, fourth):
        part = lax.bitwise_and(iota((8, first.shape[1]), 0), 3)
        return jnp.where(part == 0, first, jnp.where(part == 1, second, jnp.where(part == 2, third, fourth)))

    def main_chunk(span):
        cz, cy, cx, fz, fy, fx = place(span)
        which, low = lax.shift_right_logical(cx, fold.bit_length() - 1), lax.bitwise_and(cx, fold - 1)
        low_x[:, span] = hot_at(fold, low).astype(low_x.dtype)
        prod = dot_nn(mesh_s[...], jnp.concatenate(
            [hot_at(fold, jnp.where(which == f, low, -1)) for f in range(folds)], axis=0))
        z_at, z_frac = jnp.broadcast_to(cz, (8, chunk)), jnp.broadcast_to(fz, (8, chunk))
        gz0 = 1.0 - z_frac
        tiles = size_y // 8
        total = [[jnp.zeros((8, chunk), F32) for _ in range(tiles)] for _ in range(4)]
        for z in range(size_z):
            lower, upper = z_at == z, z_at == z - 1
            weight = jnp.where(lower, gz0, jnp.where(upper, z_frac, 0.0))
            diff = jnp.where(lower, -1.0, jnp.where(upper, 1.0, 0.0))
            for t in range(tiles):
                first = z * size_y + 8 * t
                at = [prod[q * slab + first:q * slab + first + 8] for q in range(4)]
                value, slope = at[0] + at[1], at[2] + at[3]
                total[0][t] += weight * value
                total[1][t] += diff * value
                total[2][t] += weight * slope
                total[3][t] += diff * slope
        w_y, d_y = weights(size_y, cy, fy)
        sums = [0.0, 0.0, 0.0]
        for t in range(tiles):
            a_w, a_d, b_w, b_d = (total[q][t] for q in range(4))
            w, d = w_y[8 * t:8 * t + 8], d_y[8 * t:8 * t + 8]
            sums = [sums[0] + (a_d + fx * b_d) * w, sums[1] + (a_w + fx * b_w) * d, sums[2] + b_w * w]
        for q in range(3):
            base_s[q, :, span] = sums[q]

    def top(cell, frac, size):
        at_top = cell == size - 1
        return jnp.where(at_top, frac, 0.0), jnp.where(at_top, 1.0, 0.0)

    def folded(plane):
        table = with_diff(plane)
        return jnp.concatenate([table[:, f * fold:(f + 1) * fold] for f in range(folds)], axis=0)

    def by_rows(first, second, third):
        row = iota(first.shape, 0)
        even, lower = lax.bitwise_and(row, 1) == 0, lax.bitwise_and(row, 2) == 0
        pair = jnp.where(even, first, second) + pltpu.roll(jnp.where(even, second, first), 1, 0)
        third = third + pltpu.roll(third, 1, 0)
        third = jnp.where(even, third, 0.0)
        both = jnp.where(lower, pair, third) + pltpu.roll(jnp.where(lower, third, pair), 2, 0)
        return both + pltpu.roll(both, 4, 0)

    def either(first, one, other):
        if isinstance(first, bool):
            return one if first else other
        return jnp.where(first, one, other)

    def halo_weights(span, along_y):
        cz, cy, cx, fz, fy, fx = place(span)
        size = either(along_y, size_y, size_z) if isinstance(along_y, bool) else size_y
        w, d = weights(size, either(along_y, cy, cz), either(along_y, fy, fz))
        w_top, d_top = top(either(along_y, cz, cy), either(along_y, fz, fy), either(along_y, size_z, size_y))
        across, beside = d_top * w, w_top * d
        return either(along_y, across, beside), either(along_y, beside, across), w_top * w

    def halo_sums(table, span, factors):
        cx, fx = place(span)[2::3]
        prod = dot_nn(table, low_x[:, span])
        count = table.shape[0] // folds
        size = count // 4
        which = lax.shift_right_logical(cx, fold.bit_length() - 1)

        def found(first):
            pick = None
            for f in reversed(range(folds)):
                at = f * count + first
                part = prod[at:at + size] + prod[at + size:at + 2 * size]
                pick = part if pick is None else jnp.where(which == f, part, pick)
            return pick

        value, slope = found(0), found(2 * size)
        read = value + fx * slope
        parts = (factors[0] * read, factors[1] * read, factors[2] * slope)
        sums = []
        for q in range(3):
            total = base_s[q, :, span]
            for t in range(0, size, 8):
                total = total + parts[q][t:t + 8]
            sums.append(total)
        return sums

    def about(span):
        cz, cy, cx, fz, fy, fx = place(span)
        (wz, dz), (wy, dy) = top(cz, fz, size_z), top(cy, fy, size_y)
        return by_four((slots[:, span] + 1).astype(F32), cx.astype(F32) + fx, wz * dy, wy * dz)

    def pack_rows(g, parts, wide, ranked):
        total = jnp.zeros((len(parts[0]) * wide, 2 * LANES), F32)
        for part, span in zip(parts, spans):
            mask = mine_s[:, span] if groups == 1 else own_rows(g, span)
            left = jnp.concatenate([each * mask[r:r + 16] for each in part for r in range(0, wide, 16)], axis=0)
            total = total + ranked(left, span)
        packed = total[:wide]
        for k in range(1, len(parts[0])):
            packed = packed + total[k * wide:(k + 1) * wide]
        return packed

    def keep(packed, into, first):
        for d in range(packed.shape[0] // 2):
            half, side = d // 2, d % 2 * LANES
            into[first + d, 0:4] = packed[4 * half:4 * half + 4, side:side + LANES]

    def pack(parts, into, ranked):
        def pack_group(g, carry):
            keep(pack_rows(g, parts, 2 * group, ranked), into, g * group)
            return carry

        over(groups, pack_group, 0)

    def by_rank(left, span):
        return dot_nt(left, rank_s[:, span])

    def by_rank_t(left, span):
        return dot_nn(left, rank_t[span])

    def terms_of(value, terms):
        return terms(jnp.concatenate([value] * 2, axis=0))

    pl.semaphore_wait(barrier, devices - 1)
    below_z = lax.rem(gz + count_z - 1, count_z)
    below_y = lax.rem(gy + count_y - 1, count_y)
    halos = []
    for i, (source, target, device) in enumerate((
        (row_s, halo_s.at[0, 0:size_z], (gz, below_y)),
        (grid_v.at[0], halo_s.at[1, 0:size_y], (below_z, gy)),
    )):
        halos.append(pltpu.make_async_remote_copy(
            src_ref=source, dst_ref=target, send_sem=halo_send.at[i], recv_sem=halo_recv.at[i],
            device_id=device, device_id_type=MESH,
        ))
        halos[-1].start()

    def post(source, target, send_sem, recv_sem, device):
        pltpu.make_async_remote_copy(
            src_ref=source, dst_ref=target.at[me], send_sem=send_sem, recv_sem=recv_sem,
            device_id=device, device_id_type=MESH,
        ).start()

    first_few = min(2, count_y)

    def post_first(source, *where):
        for to_y in range(first_few):
            pl.when(me != to_y)(lambda to_y=to_y: post(source.at[to_y], *where, (0, to_y)))

    def post_rest(source, *where):
        def one(to_z, to_y):
            other = to_z * count_y + to_y
            pl.when(other >= first_few)(lambda: post(source.at[other], *where, (to_z, to_y)))

        each_other(one)

    def sent(source, target, send_sem, recv_sem, count):
        at = pl.ds(0, count)
        return pltpu.make_async_remote_copy(
            src_ref=source.at[at], dst_ref=target.at[at], send_sem=send_sem, recv_sem=recv_sem,
            device_id=(below_z, below_y), device_id_type=MESH,
        )

    early = chunks // 2
    for span in spans[:early]:
        main_chunk(span)
    pack([terms_of(about(span), thirds) for span in spans], early_s, by_rank)
    shared = [corner[:, k * LANES:(k + 1) * LANES] for k in range(pieces_x)]

    def share(d, carry):
        for k in range(pieces_x):
            early_s[d, 4 + k:5 + k] = shared[k]
        return carry

    lax.fori_loop(0, devices, share, 0, unroll=devices <= 64)

    post_first(early_s, early_r, early_send, early_recv)
    post_rest(early_s, early_r, early_send, early_recv)
    early_r[me] = early_s[me]

    for span in spans:
        rank_t[span] = rank_s[:, span].T.astype(rank_t.dtype)
    for span in spans[early:]:
        main_chunk(span)

    at_end = lax.div(gy + 1, count_y)
    y_last = at_end == 1 if size_z == size_y else True
    y_copy, z_copy = halos

    def wait_for(first):
        if isinstance(first, bool):
            (z_copy if first else y_copy).wait()
        else:
            pl.when(first)(z_copy.wait)
            pl.when(jnp.logical_not(first))(y_copy.wait)

    def plane(along_y):
        if isinstance(along_y, bool):
            return folded(halo_s[1, 0:size_y] if along_y else halo_s[0, 0:size_z])
        return folded(halo_s[at_end if along_y is y_last else 1 - at_end])

    y_first = not y_last if isinstance(y_last, bool) else jnp.logical_not(y_last)
    wait_for(y_last)
    table = plane(y_last)
    for span in spans:
        sums = halo_sums(table, span, halo_weights(span, y_last))
        for q in range(3):
            base_s[q, :, span] = sums[q]
        for q, factor in enumerate(halo_weights(span, y_first)):
            last_s[q, :, span] = factor
    wait_for(y_first)
    table = plane(y_first)
    parts = [
        terms_of(by_rows(*halo_sums(table, span, [last_s[q, :, span] for q in range(3)])), split) for span in spans
    ]
    keep(pack_rows(0, parts, 16, by_rank_t), first_s, 0)
    post_first(first_s, later_r, later_send, later_recv.at[lax.div(gy, 2)])
    pack(parts, later_s, by_rank_t)
    post_rest(later_s, later_r, later_send, later_recv.at[lax.div(gy, 2)])
    later_r[me] = later_s[me]

    sent(early_s, early_r, early_send, early_recv, devices - 1).wait()

    def from_corner(source):
        info = early_r[source]
        at_z, at_y = source // count_y, source % count_y
        if isinstance(source, int):
            other = (at_z + 1) % count_z * count_y + (at_y + 1) % count_y
        else:
            other = lax.rem(at_z + 1, count_z) * count_y + lax.rem(at_y + 1, count_y)
        row = early_r[other][4:]
        row = jnp.concatenate([row, row], axis=0) if pieces_x == 4 else row
        full = row.shape[0]
        where_x = jnp.broadcast_to(info[1:2], (full, LANES))
        cell = where_x.astype(jnp.int32)
        frac = where_x - cell.astype(F32)
        part = lax.bitwise_and(iota((full, LANES), 0), pieces_x - 1)

        def read(at):
            found = jnp.take_along_axis(row, lax.bitwise_and(at, LANES - 1), axis=1, mode="promise_in_bounds")
            found = jnp.where(part == lax.shift_right_logical(at, 7), found, 0.0)
            return jnp.sum(found[:pieces_x], axis=0, keepdims=True)

        low, high = read(cell), read(lax.bitwise_and(cell + 1, size_x - 1))
        slope = high - low
        value = low + frac[0:1] * slope
        wz, wy = info[2:3], info[3:4]
        return by_four(wy * value, wz * value, wz * wy * slope, 0.0)[:4]

    def where_to(blocks):
        record = jnp.concatenate([block[0:1] for block in blocks], axis=1).astype(jnp.int32) - 1
        return (hot_at(LANES, lax.bitwise_and(record, LANES - 1)),
                hot_at(4 * highs, lax.shift_right_arithmetic(record, 7), 2))

    def added(blocks, low_hot, high_hot):
        values = jnp.concatenate(blocks, axis=1)
        halves = split(jnp.concatenate([values] * 4, axis=0))
        left = jnp.concatenate([half * high_hot[r:r + 16] for half in halves for r in range(0, 4 * highs, 16)], axis=0)
        total = dot_nt(left, low_hot)
        return total[:4 * highs] + total[4 * highs:]

    order = [z * count_y + y for first in range(0, count_y, 2) for z in range(count_z) for y in (first, first + 1)]
    if groups == 1:
        low_hot, high_hot = where_to([early_r[d] for d in order])
        place_s[...] = low_hot
        high_s[...] = high_hot
        total = added([from_corner(d) for d in order], low_hot, high_hot)
    else:
        def corner_group(g, total):
            low_hot, high_hot = where_to([early_r[g * group + d] for d in range(group)])
            return total + added([from_corner(g * group + d) for d in range(group)], low_hot, high_hot)

        total = over(groups, corner_group, jnp.zeros((4 * highs, LANES), F32))

    batch = 2 * count_z
    for part in range(count_y // 2):
        def wait_for_batch(count):
            sent(later_s, later_r, later_send, later_recv.at[part], count).wait_recv()

        pl.when(lax.div(gy, 2) == part)(lambda: wait_for_batch(batch - 1))
        pl.when(lax.div(gy, 2) != part)(lambda: wait_for_batch(batch))
        if groups == 1:
            at = slice(part * batch * LANES, (part + 1) * batch * LANES)
            sources = order[part * batch:(part + 1) * batch]
            total = total + added([later_r[d] for d in sources], place_s[:, at], high_s[:, at])
    sent(later_s, later_r, later_send, later_recv.at[0], devices - 1).wait_send()
    if groups > 1:
        def add_group(g, total):
            low_hot, high_hot = where_to([early_r[g * group + d] for d in range(group)])
            return total + added([later_r[g * group + d] for d in range(group)], low_hot, high_hot)

        total = over(groups, add_group, total)
    for h in range(highs):
        out[:, h * LANES:(h + 1) * LANES] = total[4 * h:4 * h + 3]


def body(grid_grad, cells, offsets, owners, slots):
    size_z, size_y, size_x = grid_grad.shape
    rows = cells.shape[1]
    count_y = lax.axis_size("gy")
    devices = lax.axis_size("gz") * count_y
    group = min(32, devices)
    width = devices * LANES if devices == group else LANES
    vmem = pl.BlockSpec(memory_space=pltpu.VMEM)
    hbm = pl.BlockSpec(memory_space=pltpu.HBM)
    return pl.pallas_call(
        kernel,
        out_shape=pltpu.VMEM((3, rows), F32),
        in_specs=[hbm] * 5,
        out_specs=vmem,
        scratch_shapes=[
            pltpu.VMEM((3, rows), jnp.int32),
            pltpu.VMEM((3, rows), jnp.int32),
            pltpu.VMEM((1, rows), jnp.int32),
            pltpu.VMEM((1, rows), jnp.int32),
            pltpu.VMEM((size_z, size_y, size_x), F32),
            pltpu.VMEM((size_z, size_x), F32),
            pltpu.VMEM((2, max(size_z, size_y), size_x), F32),
            pltpu.VMEM((4 * size_z * size_y, size_x), BF),
            pltpu.VMEM((min(256, size_x), rows), jnp.float8_e4m3fn),
            pltpu.VMEM((3, 8, rows), F32),
            pltpu.VMEM((3, size_z, rows), F32),
            pltpu.VMEM((2 * LANES, rows), BF),
            pltpu.VMEM((rows, 2 * LANES), jnp.float8_e4m3fn),
            pltpu.VMEM((2 * group, rows), BF),
            pltpu.VMEM((devices, 4 + size_x // LANES, LANES), F32),
            pltpu.VMEM((devices, 4, LANES), F32),
            pltpu.VMEM((8, 4, LANES), F32),
            pltpu.VMEM((devices, 4 + size_x // LANES, LANES), F32),
            pltpu.VMEM((devices, 4, LANES), F32),
            pltpu.VMEM((LANES, width), BF),
            pltpu.VMEM((4 * rows // LANES, width), BF),
            pltpu.SemaphoreType.DMA((5,)),
            pltpu.SemaphoreType.DMA((2,)),
            pltpu.SemaphoreType.DMA((2,)),
            pltpu.SemaphoreType.DMA,
            pltpu.SemaphoreType.DMA,
            pltpu.SemaphoreType.DMA,
            pltpu.SemaphoreType.DMA((count_y // 2,)),
        ],
        compiler_params=pltpu.CompilerParams(collective_id=0, has_side_effects=True, vmem_limit_bytes=56 * 1024 * 1024),
        name="cic",
    )(grid_grad, cells, offsets, owners.reshape(1, rows), slots.reshape(1, rows))


def solution(mesh):
    placed = (
        P("gz", "gy", None),
        P(None, ("gz", "gy")),
        P(None, ("gz", "gy")),
        P(("gz", "gy"), None),
        P(("gz", "gy")),
    )
    return jax.shard_map(
        body, mesh=mesh, in_specs=placed, out_specs=P(None, ("gz", "gy")), check_vma=False
    )
```

```python
import jax
import jax.numpy as jnp
from jax import lax
from jax.experimental import pallas as pl
from jax.experimental.pallas import tpu as pltpu
from jax.sharding import PartitionSpec as P

MESH = pl.DeviceIdType.MESH
BF = jnp.bfloat16
F32 = jnp.float32
LANES = 128


def iota(shape, axis):
    return lax.broadcasted_iota(jnp.int32, shape, axis)


def hot(mask):
    return jnp.where(mask, 1.0, 0.0).astype(BF)


def split(value):
    high = value.astype(BF)
    low = (value - high.astype(F32)).astype(BF)
    return high, low


def dot_nn(a, b):
    return lax.dot_general(a, b, (((1,), (0,)), ((), ())), preferred_element_type=F32)


def dot_nt(a, b):
    return lax.dot_general(a, b, (((1,), (1,)), ((), ())), preferred_element_type=F32)


def with_diff(rows):
    size_x = rows.shape[1]
    diff = pltpu.roll(rows, size_x - 1, 1) - rows
    return jnp.concatenate([*split(rows), *split(diff)], axis=0)


def hot_at(size, value, shift=0):
    value = jnp.broadcast_to(value.astype(F32), (16, value.shape[1])).astype(BF)
    at = lax.shift_right_logical(iota(value.shape, 0), shift).astype(F32)
    one, none = jnp.ones(value.shape, BF), jnp.zeros(value.shape, BF)
    return jnp.concatenate(
        [jnp.where((at + float(k >> shift)).astype(BF) == value, one, none) for k in range(0, size, 16)], axis=0)


def thirds(value):
    high, rest = split(value)
    return high, rest, (value - high.astype(F32) - rest.astype(F32)).astype(BF)


def over(count, step, carry):
    if count == 1:
        return step(0, carry)
    return lax.fori_loop(0, count, step, carry)


def kernel(
    grid_ref, cells_ref, offsets_ref, owners_ref, slots_ref, out,
    cells, offsets, owners, slots, grid_v, row_s, halo_s, mesh_s, low_x, base_s, last_s, rank_s, rank_t, mine_s, early_s, later_s,
    first_s,
    early_r, later_r, place_s, high_s, load_sem, halo_send, halo_recv, early_send, early_recv, later_send, later_recv,
):
    count_z, count_y = lax.axis_size("gz"), lax.axis_size("gy")
    devices = count_z * count_y
    gz, gy = lax.axis_index("gz"), lax.axis_index("gy")
    me = gz * count_y + gy
    size_z, size_y, size_x = grid_ref.shape
    rows = cells.shape[1]
    chunk = min(256, rows)
    chunks = rows // chunk
    spans = [pl.ds(j * chunk, chunk) for j in range(chunks)]
    group = min(32, devices)
    groups = devices // group
    slab = size_z * size_y
    pieces_x = size_x // LANES
    fold = low_x.shape[0]
    folds = size_x // fold
    highs = rows // LANES

    loads = []
    for i, (source, target) in enumerate((
        (owners_ref, owners), (grid_ref, grid_v), (cells_ref, cells), (offsets_ref, offsets), (slots_ref, slots),
    )):
        loads.append(pltpu.make_async_copy(source, target, load_sem.at[i]))
        loads[-1].start()
    barrier = pltpu.get_barrier_semaphore()

    def each_other(act):
        few = devices <= 64

        def along_y(to_z, first):
            def step(shift, carry):
                act(to_z, lax.rem(gy + shift, count_y))
                return carry
            lax.fori_loop(first, count_y, step, 0, unroll=few)

        def step_z(shift, carry):
            along_y(lax.rem(gz + shift, count_z), 0)
            return carry
        along_y(gz, 1)
        lax.fori_loop(1, count_z, step_z, 0, unroll=few)

    def greet(to_z, to_y):
        pl.semaphore_signal(barrier, inc=1, device_id=(to_z, to_y), device_id_type=MESH)

    each_other(greet)

    loads[0].wait()
    owner = owners[...]
    before = hot(iota((chunk, chunk), 0) < iota((chunk, chunk), 1))

    def rank_group(g, ranks):
        mine = jnp.where(iota((group, rows), 0) + g * group == owner, 1.0, 0.0)
        pieces = [mine[:, c * chunk:(c + 1) * chunk] for c in range(chunks)]
        inside = dot_nn(jnp.concatenate(pieces, axis=0).astype(BF), before)
        start = jnp.zeros((group, 1), F32)
        found = []
        for c in range(chunks):
            where = inside[c * group:(c + 1) * group] + start
            found.append(jnp.sum(pieces[c] * where, axis=0, keepdims=True))
            start = start + jnp.sum(pieces[c], axis=1, keepdims=True)
        return ranks + jnp.concatenate(found, axis=1)

    ranks = over(groups, rank_group, jnp.zeros((1, rows), F32))
    odd = lax.bitwise_and(owner, 1)
    rank_s[...] = hot_at(2 * LANES, ranks + (odd * LANES).astype(F32))

    def own_rows(g, span):
        return hot_at(2 * group, lax.shift_right_logical(owners[:, span], 1) - g * (group // 2), 2)

    if groups == 1:
        mine_s[...] = own_rows(0, pl.ds(0, rows))

    for copy in loads[1:]:
        copy.wait()
    row_s[...] = grid_v[:, 0, :]
    mesh_s[...] = with_diff(grid_v[...].reshape(slab, size_x))
    corner = grid_v[0, 0:1, :]

    def place(span):
        cell = cells[:, span]
        frac = (offsets[:, span].astype(F32) + 0.5) / 1024.0
        return (cell[0:1] - gz * size_z, cell[1:2] - gy * size_y, cell[2:3],
                frac[0:1], frac[1:2], frac[2:3])

    def weights(size, cell, frac):
        at = iota((size, cell.shape[1]), 0)
        lower, upper = at == cell, at == cell + 1
        return (jnp.where(lower, 1.0 - frac, jnp.where(upper, frac, 0.0)),
                jnp.where(lower, -1.0, jnp.where(upper, 1.0, 0.0)))

    def by_four(first, second, third, fourth):
        part = lax.bitwise_and(iota((8, first.shape[1]), 0), 3)
        return jnp.where(part == 0, first, jnp.where(part == 1, second, jnp.where(part == 2, third, fourth)))

    def main_chunk(span):
        cz, cy, cx, fz, fy, fx = place(span)
        which, low = lax.shift_right_logical(cx, fold.bit_length() - 1), lax.bitwise_and(cx, fold - 1)
        low_x[:, span] = hot_at(fold, low).astype(low_x.dtype)
        prod = dot_nn(mesh_s[...], jnp.concatenate(
            [hot_at(fold, jnp.where(which == f, low, -1)) for f in range(folds)], axis=0))
        z_at, z_frac = jnp.broadcast_to(cz, (8, chunk)), jnp.broadcast_to(fz, (8, chunk))
        gz0 = 1.0 - z_frac
        tiles = size_y // 8
        total = [[jnp.zeros((8, chunk), F32) for _ in range(tiles)] for _ in range(4)]
        for z in range(size_z):
            lower, upper = z_at == z, z_at == z - 1
            weight = jnp.where(lower, gz0, jnp.where(upper, z_frac, 0.0))
            diff = jnp.where(lower, -1.0, jnp.where(upper, 1.0, 0.0))
            for t in range(tiles):
                first = z * size_y + 8 * t
                at = [prod[q * slab + first:q * slab + first + 8] for q in range(4)]
                value, slope = at[0] + at[1], at[2] + at[3]
                total[0][t] += weight * value
                total[1][t] += diff * value
                total[2][t] += weight * slope
                total[3][t] += diff * slope
        w_y, d_y = weights(size_y, cy, fy)
        sums = [0.0, 0.0, 0.0]
        for t in range(tiles):
            a_w, a_d, b_w, b_d = (total[q][t] for q in range(4))
            w, d = w_y[8 * t:8 * t + 8], d_y[8 * t:8 * t + 8]
            sums = [sums[0] + (a_d + fx * b_d) * w, sums[1] + (a_w + fx * b_w) * d, sums[2] + b_w * w]
        for q in range(3):
            base_s[q, :, span] = sums[q]

    def top(cell, frac, size):
        at_top = cell == size - 1
        return jnp.where(at_top, frac, 0.0), jnp.where(at_top, 1.0, 0.0)

    def folded(plane):
        table = with_diff(plane)
        return jnp.concatenate([table[:, f * fold:(f + 1) * fold] for f in range(folds)], axis=0)

    def by_rows(first, second, third):
        row = iota(first.shape, 0)
        even, lower = lax.bitwise_and(row, 1) == 0, lax.bitwise_and(row, 2) == 0
        pair = jnp.where(even, first, second) + pltpu.roll(jnp.where(even, second, first), 1, 0)
        third = third + pltpu.roll(third, 1, 0)
        third = jnp.where(even, third, 0.0)
        both = jnp.where(lower, pair, third) + pltpu.roll(jnp.where(lower, third, pair), 2, 0)
        return both + pltpu.roll(both, 4, 0)

    def either(first, one, other):
        if isinstance(first, bool):
            return one if first else other
        return jnp.where(first, one, other)

    def halo_weights(span, along_y):
        cz, cy, cx, fz, fy, fx = place(span)
        size = either(along_y, size_y, size_z) if isinstance(along_y, bool) else size_y
        w, d = weights(size, either(along_y, cy, cz), either(along_y, fy, fz))
        w_top, d_top = top(either(along_y, cz, cy), either(along_y, fz, fy), either(along_y, size_z, size_y))
        across, beside = d_top * w, w_top * d
        return either(along_y, across, beside), either(along_y, beside, across), w_top * w

    def halo_sums(table, span, factors):
        cx, fx = place(span)[2::3]
        prod = dot_nn(table, low_x[:, span])
        count = table.shape[0] // folds
        size = count // 4
        which = lax.shift_right_logical(cx, fold.bit_length() - 1)

        def found(first):
            pick = None
            for f in reversed(range(folds)):
                at = f * count + first
                part = prod[at:at + size] + prod[at + size:at + 2 * size]
                pick = part if pick is None else jnp.where(which == f, part, pick)
            return pick

        value, slope = found(0), found(2 * size)
        read = value + fx * slope
        parts = (factors[0] * read, factors[1] * read, factors[2] * slope)
        sums = []
        for q in range(3):
            total = base_s[q, :, span]
            for t in range(0, size, 8):
                total = total + parts[q][t:t + 8]
            sums.append(total)
        return sums

    def about(span):
        cz, cy, cx, fz, fy, fx = place(span)
        (wz, dz), (wy, dy) = top(cz, fz, size_z), top(cy, fy, size_y)
        return by_four((slots[:, span] + 1).astype(F32), cx.astype(F32) + fx, wz * dy, wy * dz)

    def pack_rows(g, parts, wide, ranked):
        total = jnp.zeros((len(parts[0]) * wide, 2 * LANES), F32)
        for part, span in zip(parts, spans):
            mask = mine_s[:, span] if groups == 1 else own_rows(g, span)
            left = jnp.concatenate([each * mask[r:r + 16] for each in part for r in range(0, wide, 16)], axis=0)
            total = total + ranked(left, span)
        packed = total[:wide]
        for k in range(1, len(parts[0])):
            packed = packed + total[k * wide:(k + 1) * wide]
        return packed

    def keep(packed, into, first):
        for d in range(packed.shape[0] // 2):
            half, side = d // 2, d % 2 * LANES
            into[first + d, 0:4] = packed[4 * half:4 * half + 4, side:side + LANES]

    def pack(parts, into, ranked):
        def pack_group(g, carry):
            keep(pack_rows(g, parts, 2 * group, ranked), into, g * group)
            return carry

        over(groups, pack_group, 0)

    def by_rank(left, span):
        return dot_nt(left, rank_s[:, span])

    def by_rank_t(left, span):
        return dot_nn(left, rank_t[span])

    def terms_of(value, terms):
        return terms(jnp.concatenate([value] * 2, axis=0))

    pl.semaphore_wait(barrier, devices - 1)
    below_z = lax.rem(gz + count_z - 1, count_z)
    below_y = lax.rem(gy + count_y - 1, count_y)
    halos = []
    for i, (source, target, device) in enumerate((
        (row_s, halo_s.at[0, 0:size_z], (gz, below_y)),
        (grid_v.at[0], halo_s.at[1, 0:size_y], (below_z, gy)),
    )):
        halos.append(pltpu.make_async_remote_copy(
            src_ref=source, dst_ref=target, send_sem=halo_send.at[i], recv_sem=halo_recv.at[i],
            device_id=device, device_id_type=MESH,
        ))
        halos[-1].start()

    def post(source, target, send_sem, recv_sem, device):
        pltpu.make_async_remote_copy(
            src_ref=source, dst_ref=target.at[me], send_sem=send_sem, recv_sem=recv_sem,
            device_id=device, device_id_type=MESH,
        ).start()

    first_few = min(2, count_y)

    def post_first(source, *where):
        for to_y in range(first_few):
            pl.when(me != to_y)(lambda to_y=to_y: post(source.at[to_y], *where, (0, to_y)))

    def post_rest(source, *where):
        def one(to_z, to_y):
            other = to_z * count_y + to_y
            pl.when(other >= first_few)(lambda: post(source.at[other], *where, (to_z, to_y)))

        each_other(one)

    def sent(source, target, send_sem, recv_sem, count):
        at = pl.ds(0, count)
        return pltpu.make_async_remote_copy(
            src_ref=source.at[at], dst_ref=target.at[at], send_sem=send_sem, recv_sem=recv_sem,
            device_id=(below_z, below_y), device_id_type=MESH,
        )

    early = chunks // 2
    for span in spans[:early]:
        main_chunk(span)
    pack([terms_of(about(span), thirds) for span in spans], early_s, by_rank)
    shared = [corner[:, k * LANES:(k + 1) * LANES] for k in range(pieces_x)]

    def share(d, carry):
        for k in range(pieces_x):
            early_s[d, 4 + k:5 + k] = shared[k]
        return carry

    lax.fori_loop(0, devices, share, 0, unroll=devices <= 64)

    post_first(early_s, early_r, early_send, early_recv)
    post_rest(early_s, early_r, early_send, early_recv)
    early_r[me] = early_s[me]

    for span in spans:
        rank_t[span] = rank_s[:, span].T.astype(rank_t.dtype)
    for span in spans[early:]:
        main_chunk(span)

    at_end = lax.div(gy + 1, count_y)
    y_last = at_end == 1 if size_z == size_y else True
    y_copy, z_copy = halos

    def wait_for(first):
        if isinstance(first, bool):
            (z_copy if first else y_copy).wait()
        else:
            pl.when(first)(z_copy.wait)
            pl.when(jnp.logical_not(first))(y_copy.wait)

    def plane(along_y):
        if isinstance(along_y, bool):
            return folded(halo_s[1, 0:size_y] if along_y else halo_s[0, 0:size_z])
        return folded(halo_s[at_end if along_y is y_last else 1 - at_end])

    y_first = not y_last if isinstance(y_last, bool) else jnp.logical_not(y_last)
    wait_for(y_last)
    table = plane(y_last)
    for span in spans:
        sums = halo_sums(table, span, halo_weights(span, y_last))
        for q in range(3):
            base_s[q, :, span] = sums[q]
        for q, factor in enumerate(halo_weights(span, y_first)):
            last_s[q, :, span] = factor
    wait_for(y_first)
    table = plane(y_first)
    parts = [
        terms_of(by_rows(*halo_sums(table, span, [last_s[q, :, span] for q in range(3)])), split) for span in spans
    ]
    keep(pack_rows(0, parts, 16, by_rank_t), first_s, 0)
    post_first(first_s, later_r, later_send, later_recv.at[lax.div(gy, 2)])
    pack(parts, later_s, by_rank_t)
    post_rest(later_s, later_r, later_send, later_recv.at[lax.div(gy, 2)])
    later_r[me] = later_s[me]

    sent(early_s, early_r, early_send, early_recv, devices - 1).wait()

    def from_corner(source):
        info = early_r[source]
        at_z, at_y = source // count_y, source % count_y
        if isinstance(source, int):
            other = (at_z + 1) % count_z * count_y + (at_y + 1) % count_y
        else:
            other = lax.rem(at_z + 1, count_z) * count_y + lax.rem(at_y + 1, count_y)
        row = early_r[other][4:]
        row = jnp.concatenate([row, row], axis=0) if pieces_x == 4 else row
        full = row.shape[0]
        where_x = jnp.broadcast_to(info[1:2], (full, LANES))
        cell = where_x.astype(jnp.int32)
        frac = where_x - cell.astype(F32)
        part = lax.bitwise_and(iota((full, LANES), 0), pieces_x - 1)

        def read(at):
            found = jnp.take_along_axis(row, lax.bitwise_and(at, LANES - 1), axis=1, mode="promise_in_bounds")
            found = jnp.where(part == lax.shift_right_logical(at, 7), found, 0.0)
            return jnp.sum(found[:pieces_x], axis=0, keepdims=True)

        low, high = read(cell), read(lax.bitwise_and(cell + 1, size_x - 1))
        slope = high - low
        value = low + frac[0:1] * slope
        wz, wy = info[2:3], info[3:4]
        return by_four(wy * value, wz * value, wz * wy * slope, 0.0)[:4]

    def where_to(blocks):
        record = jnp.concatenate([block[0:1] for block in blocks], axis=1).astype(jnp.int32) - 1
        return (hot_at(LANES, lax.bitwise_and(record, LANES - 1)),
                hot_at(4 * highs, lax.shift_right_arithmetic(record, 7), 2))

    def added(blocks, low_hot, high_hot):
        values = jnp.concatenate(blocks, axis=1)
        halves = split(jnp.concatenate([values] * 4, axis=0))
        left = jnp.concatenate([half * high_hot[r:r + 16] for half in halves for r in range(0, 4 * highs, 16)], axis=0)
        total = dot_nt(left, low_hot)
        return total[:4 * highs] + total[4 * highs:]

    order = [z * count_y + y for first in range(0, count_y, 2) for z in range(count_z) for y in (first, first + 1)]
    if groups == 1:
        low_hot, high_hot = where_to([early_r[d] for d in order])
        place_s[...] = low_hot.astype(place_s.dtype)
        high_s[...] = high_hot
        total = added([from_corner(d) for d in order], low_hot, high_hot)
    else:
        def corner_group(g, total):
            low_hot, high_hot = where_to([early_r[g * group + d] for d in range(group)])
            return total + added([from_corner(g * group + d) for d in range(group)], low_hot, high_hot)

        total = over(groups, corner_group, jnp.zeros((4 * highs, LANES), F32))

    batch = 2 * count_z
    for part in range(count_y // 2):
        def wait_for_batch(count):
            sent(later_s, later_r, later_send, later_recv.at[part], count).wait_recv()

        pl.when(lax.div(gy, 2) == part)(lambda: wait_for_batch(batch - 1))
        pl.when(lax.div(gy, 2) != part)(lambda: wait_for_batch(batch))
        if groups == 1:
            at = slice(part * batch * LANES, (part + 1) * batch * LANES)
            sources = order[part * batch:(part + 1) * batch]
            total = total + added([later_r[d] for d in sources], place_s[:, at], high_s[:, at])
    sent(later_s, later_r, later_send, later_recv.at[0], devices - 1).wait_send()
    if groups > 1:
        def add_group(g, total):
            low_hot, high_hot = where_to([early_r[g * group + d] for d in range(group)])
            return total + added([later_r[g * group + d] for d in range(group)], low_hot, high_hot)

        total = over(groups, add_group, total)
    for h in range(highs):
        out[:, h * LANES:(h + 1) * LANES] = total[4 * h:4 * h + 3]


def body(grid_grad, cells, offsets, owners, slots):
    size_z, size_y, size_x = grid_grad.shape
    rows = cells.shape[1]
    count_y = lax.axis_size("gy")
    devices = lax.axis_size("gz") * count_y
    group = min(32, devices)
    width = devices * LANES if devices == group else LANES
    vmem = pl.BlockSpec(memory_space=pltpu.VMEM)
    hbm = pl.BlockSpec(memory_space=pltpu.HBM)
    return pl.pallas_call(
        kernel,
        out_shape=pltpu.VMEM((3, rows), F32),
        in_specs=[hbm] * 5,
        out_specs=vmem,
        scratch_shapes=[
            pltpu.VMEM((3, rows), jnp.int32),
            pltpu.VMEM((3, rows), jnp.int32),
            pltpu.VMEM((1, rows), jnp.int32),
            pltpu.VMEM((1, rows), jnp.int32),
            pltpu.VMEM((size_z, size_y, size_x), F32),
            pltpu.VMEM((size_z, size_x), F32),
            pltpu.VMEM((2, max(size_z, size_y), size_x), F32),
            pltpu.VMEM((4 * size_z * size_y, size_x), BF),
            pltpu.VMEM((min(256, size_x), rows), jnp.float8_e4m3fn),
            pltpu.VMEM((3, 8, rows), F32),
            pltpu.VMEM((3, size_z, rows), F32),
            pltpu.VMEM((2 * LANES, rows), BF),
            pltpu.VMEM((rows, 2 * LANES), jnp.float8_e4m3fn),
            pltpu.VMEM((2 * group, rows), BF),
            pltpu.VMEM((devices, 4 + size_x // LANES, LANES), F32),
            pltpu.VMEM((devices, 4, LANES), F32),
            pltpu.VMEM((8, 4, LANES), F32),
            pltpu.VMEM((devices, 4 + size_x // LANES, LANES), F32),
            pltpu.VMEM((devices, 4, LANES), F32),
            pltpu.VMEM((LANES, width), jnp.float8_e4m3fn),
            pltpu.VMEM((4 * rows // LANES, width), BF),
            pltpu.SemaphoreType.DMA((5,)),
            pltpu.SemaphoreType.DMA((2,)),
            pltpu.SemaphoreType.DMA((2,)),
            pltpu.SemaphoreType.DMA,
            pltpu.SemaphoreType.DMA,
            pltpu.SemaphoreType.DMA,
            pltpu.SemaphoreType.DMA((count_y // 2,)),
        ],
        compiler_params=pltpu.CompilerParams(collective_id=0, has_side_effects=True, vmem_limit_bytes=56 * 1024 * 1024),
        name="cic",
    )(grid_grad, cells, offsets, owners.reshape(1, rows), slots.reshape(1, rows))


def solution(mesh):
    placed = (
        P("gz", "gy", None),
        P(None, ("gz", "gy")),
        P(None, ("gz", "gy")),
        P(("gz", "gy"), None),
        P(("gz", "gy")),
    )
    return jax.shard_map(
        body, mesh=mesh, in_specs=placed, out_specs=P(None, ("gz", "gy")), check_vma=False
    )
```
